32 devices in a mesh: section: 4 (over y, core), row: 8 (over z, x).
Axes of the slice: x: 2, y: 2, z: 4, core: 2. Of those that a mesh axis runs over, the one named last changes fastest.
Arguments:
- diag_blocks: float32 [4, 2, 8, 256, 256], P('section', None, 'row'), may hold values from -9 to 9, as said below
- coupling_blocks: float32 [4, 2, 8, 256, 256], P('section', None, 'row'), as said below
Outputs:
- reduced_diag: float32 [4, 2, 8, 256, 256], P('section', None, 'row')
- reduced_coupling: float32 [4, 2, 8, 256, 256], P('section', None, 'row')
The draws below stay inside these ranges and needn't reach their ends.
Inputs may be any that keep to these rules, and one draw needn't show every extreme that they name: `diag_blocks`: every block is symmetric. `coupling_blocks`: every block is three times the identity plus a random part whose entries are at most 5 / sqrt(256) in magnitude and whose spectral norm is at most 2.5, so every block is invertible.
All inputs are finite; a program needn't handle non-finite values.
Results may differ from the reference program's by a relative error of at most 0.0003.
Values sent between devices are 32-bit elements; how exact they have to be, the bound alone decides.
A program may use at most 64 MiB of HBM per device.

```python
import jax
import jax.numpy as jnp
from jax import lax

D = 256
MB = 2
NBLK = 8
GROUPS = 4


def draw_diag_blocks(key, part):
    full_shape = (GROUPS, MB, NBLK, D, D)
    random_part = jnp.clip(jax.random.normal(key, full_shape, jnp.float32), -6.0, 6.0)
    return (random_part + jnp.swapaxes(random_part, -1, -2)) * 0.7071


def draw_coupling_blocks(key, part):
    full_shape = (GROUPS, MB, NBLK, D, D)
    random_part = jnp.clip(jax.random.normal(key, full_shape, jnp.float32), -5.0, 5.0)
    identity = jnp.eye(D, dtype=jnp.float32)
    return 3.0 * identity + random_part / jnp.sqrt(jnp.float32(D))


def setup_inputs(seed: int = 0) -> dict:
    arg_keys = jax.random.split(jax.random.key(seed), 3)
    return {
        "diag_blocks": draw_diag_blocks(jax.random.fold_in(arg_keys[2], 71), 0),
        "coupling_blocks": draw_coupling_blocks(jax.random.fold_in(arg_keys[2], 71), 0),
    }


highest = lax.Precision.HIGHEST

def product(left, right):
    return jnp.dot(left.astype(jnp.float32), right.astype(jnp.float32), precision=highest, preferred_element_type=jnp.float32)

def qfactor(panel_now):
    gram_first = product(panel_now.T, panel_now)
    lower_first = jnp.linalg.cholesky(gram_first)
    first_pass = jax.scipy.linalg.solve_triangular(lower_first, panel_now.T, lower=True).T
    gram_second = product(first_pass.T, first_pass)
    lower_second = jnp.linalg.cholesky(gram_second)
    orthogonal = jax.scipy.linalg.solve_triangular(lower_second, first_pass.T, lower=True).T
    upper_part = product(lower_second.T, lower_first.T)
    return (orthogonal, upper_part)

def sweep_matrix(diagonal, coupling):
    identity = jnp.eye(D, dtype=jnp.float32)

    def sweep_step(previous, blocks_pair):
        diag_now, coupling_now = blocks_pair
        panel_now = product(coupling_now, previous)
        orthogonal, upper_part = qfactor(panel_now)
        new_diag = product(product(orthogonal.T, diag_now), orthogonal)
        return (orthogonal, (new_diag, upper_part))
    unused, outputs = lax.scan(sweep_step, identity, (diagonal, coupling))
    return outputs

def reference(diag_blocks, coupling_blocks):
    flat_diag = diag_blocks.reshape(GROUPS * MB, NBLK, D, D)
    flat_coupling = coupling_blocks.reshape(GROUPS * MB, NBLK, D, D)
    new_diag, triangles = jax.vmap(sweep_matrix)(flat_diag, flat_coupling)
    new_diag = new_diag.reshape(GROUPS, MB, NBLK, D, D)
    triangles = triangles.reshape(GROUPS, MB, NBLK, D, D)
    return (new_diag, triangles)
```

```python
import jax
import jax.numpy as jnp
from jax import lax
from jax.experimental import pallas as pl
from jax.experimental.pallas import tpu as pltpu
from jax.sharding import PartitionSpec as P

highest = lax.Precision.HIGHEST
f32, bf16 = jnp.float32, jnp.bfloat16

DAMP, COARSE, FINE = 5.0, 0.5, 2e-3
COARSE_STEPS, FINE_STEPS = 48, 8
BELOW = 5e-5


def split(value):
    high = value.astype(bf16)
    return high, (value - high.astype(f32)).astype(bf16)


def dot_nn(left, right):
    return lax.dot_general(left, right, (((1,), (0,)), ((), ())), preferred_element_type=f32)


def dot_nt(left, right):
    return lax.dot_general(left, right, (((1,), (1,)), ((), ())), preferred_element_type=f32)


def fine_dot(dot, left, right):
    left_high, left_low = split(left)
    right_high, right_low = split(right)
    return dot(left_high, right_high) + (dot(left_high, right_low) + dot(left_low, right_high))


def newton_kernel(panel_ref, factor_ref, error_ref, tri_ref):
    count, order = panel_ref.shape[0], panel_ref.shape[1]
    rows = lax.broadcasted_iota(jnp.int32, (order, order), 0)
    cols = lax.broadcasted_iota(jnp.int32, (order, order), 1)
    eye = (rows == cols).astype(f32)
    half = jnp.where(rows > cols, 1.0, 0.5 * eye).astype(f32)

    for m in range(count):
        panel = panel_ref[m]
        scale = lax.rsqrt(jnp.sum(panel * panel, axis=1, keepdims=True))
        factor_ref[m] = panel * scale
        tri_ref[m] = eye * scale

    def coarse(carried):
        step, worst = carried
        worst = jnp.float32(0.0)
        for m in range(count):
            near = factor_ref[m].astype(bf16)
            lower = (dot_nt(near, near) - eye) * half
            size2 = jnp.sum(lower * lower)
            move = (lower * jnp.minimum(1.0, DAMP * lax.rsqrt(size2))).astype(bf16)
            factor_ref[m] -= dot_nn(move, near)
            tri_ref[m] -= dot_nn(move, tri_ref[m].astype(bf16))
            worst = jnp.maximum(worst, 2.0 * size2)
        return step + 1, worst

    lax.while_loop(
        lambda c: (c[0] < COARSE_STEPS) & (c[1] > COARSE * COARSE), coarse, (jnp.int32(0), jnp.float32(1e9))
    )
    for m in range(count):
        factor_ref[m] = fine_dot(dot_nn, tri_ref[m], panel_ref[m])

    def fine(carried):
        step, worst = carried
        worst = jnp.float32(0.0)
        for m in range(count):
            near = factor_ref[m]
            lower = (fine_dot(dot_nt, near, near) - eye) * half
            factor_ref[m] = near - fine_dot(dot_nn, lower, near)
            worst = jnp.maximum(worst, 2.0 * jnp.sum(lower * lower))
        return step + 1, worst

    _, worst = lax.while_loop(
        lambda c: (c[0] < FINE_STEPS) & (c[1] > FINE * FINE), fine, (jnp.int32(0), jnp.float32(1e9))
    )
    error_ref[...] = jnp.full(error_ref.shape, worst, f32)


def orthogonal_rows(panel):
    return pl.pallas_call(
        newton_kernel,
        out_shape=(jax.ShapeDtypeStruct(panel.shape, f32), jax.ShapeDtypeStruct((8, 128), f32)),
        in_specs=[pl.BlockSpec(memory_space=pltpu.VMEM)],
        out_specs=(pl.BlockSpec(memory_space=pltpu.VMEM), pl.BlockSpec(memory_space=pltpu.VMEM)),
        scratch_shapes=[pltpu.VMEM(panel.shape, f32)],
        cost_estimate=pl.CostEstimate(flops=10**9, bytes_accessed=10**6, transcendentals=0),
    )(panel)


def close_dot(spec, left, right):
    return jnp.einsum(spec, left, right, precision=lax.Precision.HIGH, preferred_element_type=f32)


def prefix_sweep(diagonal, coupling):
    count = lax.axis_size("row")
    position = lax.axis_index("row")
    order = coupling.shape[-1]
    product_t = jnp.swapaxes(coupling, -1, -2)
    reach = 1
    while reach < count:
        before = shifted(product_t, "row", reach)
        product_t = jnp.where(position >= reach, close_dot("bij,bjk->bik", before, product_t), product_t)
        reach *= 2
    factor_t, error = orthogonal_rows(product_t)
    eye = jnp.broadcast_to(jnp.eye(order, dtype=f32), factor_t.shape)
    before = jnp.where(position == 0, eye, shifted(factor_t, "row", 1))
    turned = close_dot("bij,bjk->bik", factor_t, coupling)
    new_diag = close_dot("bij,bkj->bik", close_dot("bij,bjk->bik", factor_t, diagonal), factor_t)
    full = close_dot("bij,bkj->bik", turned, before)
    upper = jnp.triu(full)
    below2 = jnp.sum((full - upper) ** 2)
    all2 = jnp.sum(full**2)
    sound = (error[0, 0] <= FINE * FINE) & (below2 <= BELOW * BELOW * all2)
    sound = sound & jnp.all(jnp.diagonal(full, axis1=-2, axis2=-1) > 0.0)
    return new_diag, upper, 1.0 - sound.astype(f32), below2 / all2, error[0, 0]


def shards(diag_blocks, coupling_blocks):
    if diag_blocks.shape[2] != 1:
        return chain(diag_blocks, coupling_blocks)
    new_diag, upper, fault, _, _ = prefix_sweep(diag_blocks[0, :, 0], coupling_blocks[0, :, 0])
    faults = lax.psum(fault, ("section", "row"))
    return lax.cond(
        faults == 0.0,
        lambda: (new_diag[None, :, None], upper[None, :, None]),
        lambda: chain(diag_blocks, coupling_blocks),
    )


def shifted(block, axis, distance):
    devices = range(lax.axis_size(axis))
    route = [(i - distance, i) for i in devices if i - distance in devices]
    return lax.ppermute(block, axis, route)


def product(left, right):
    return jnp.dot(left, right, precision=highest, preferred_element_type=jnp.float32)


def qfactor(panel_now):
    gram_first = product(panel_now.T, panel_now)
    lower_first = jnp.linalg.cholesky(gram_first)
    first_pass = jax.scipy.linalg.solve_triangular(lower_first, panel_now.T, lower=True).T
    gram_second = product(first_pass.T, first_pass)
    lower_second = jnp.linalg.cholesky(gram_second)
    orthogonal = jax.scipy.linalg.solve_triangular(lower_second, first_pass.T, lower=True).T
    upper_part = product(lower_second.T, lower_first.T)
    return (orthogonal, upper_part)


def segment(panel_now, diagonal):
    orthogonal, upper_part = qfactor(panel_now)
    new_diag = [product(product(orthogonal.T, diagonal[0]), orthogonal)]
    triangles = [upper_part]
    return (jnp.stack(new_diag), jnp.stack(triangles), orthogonal)


def pass_on(outgoing):
    return shifted(outgoing, "row", 1)


def chain(diag_blocks, coupling_blocks):
    diagonal = diag_blocks[0]
    coupling = coupling_blocks[0]
    batch_count = diagonal.shape[0]
    row_count = lax.axis_size("row")
    position = lax.axis_index("row")
    leading = position == 0

    def opening(incoming, own_first):
        made = product(own_first, incoming)
        return jnp.where(leading, own_first, made)

    new_start = jnp.zeros_like(diagonal)
    tri_start = jnp.zeros_like(diagonal)

    def process_one(incoming, new_all, tri_all, clipped):
        diag_now = lax.dynamic_index_in_dim(diagonal, clipped, 0, keepdims=False)
        coupling_now = lax.dynamic_index_in_dim(coupling, clipped, 0, keepdims=False)
        first_panel = opening(incoming, coupling_now[0])
        new_diag, triangles, last_factor = segment(first_panel, diag_now)
        new_all = lax.dynamic_update_index_in_dim(new_all, new_diag, clipped, 0)
        tri_all = lax.dynamic_update_index_in_dim(tri_all, triangles, clipped, 0)
        return (new_all, tri_all, last_factor)

    def round_step(step_number, carried):
        incoming, new_all, tri_all, outgoing = carried
        batch_index = step_number - position
        active = (batch_index >= 0) & (batch_index < batch_count)
        clipped = jnp.clip(batch_index, 0, batch_count - 1)
        new_all, tri_all, outgoing = lax.cond(
            active,
            lambda: process_one(incoming, new_all, tri_all, clipped),
            lambda: (new_all, tri_all, outgoing),
        )
        return (pass_on(outgoing), new_all, tri_all, outgoing)

    message_start = jnp.zeros_like(coupling[0, 0])
    carried = lax.fori_loop(
        0,
        row_count + batch_count - 1,
        round_step,
        (message_start, new_start, tri_start, message_start),
    )
    return (carried[1][None], carried[2][None])


def solution(mesh):
    placed = (P("section", None, "row", None, None), P("section", None, "row", None, None))
    return jax.shard_map(
        shards,
        mesh=mesh,
        in_specs=placed,
        out_specs=(P("section", None, "row", None, None), P("section", None, "row", None, None)),
        check_vma=False,
    )
```

```python
import jax
import jax.numpy as jnp
from jax import lax
from jax.experimental import pallas as pl
from jax.experimental.pallas import tpu as pltpu
from jax.sharding import PartitionSpec as P

highest = lax.Precision.HIGHEST
f32, bf16 = jnp.float32, jnp.bfloat16
MESH = pl.DeviceIdType.MESH
CHUNK = 32

DAMP, COARSE, FINE = 5.0, 0.5, 2e-3
COARSE_STEPS, FINE_STEPS = 48, 8
BELOW = 5e-5


def split(value):
    high = value.astype(bf16)
    return high, (value - high.astype(f32)).astype(bf16)


def dot_nn(left, right):
    return lax.dot_general(left, right, (((1,), (0,)), ((), ())), preferred_element_type=f32)


def dot_nt(left, right):
    return lax.dot_general(left, right, (((1,), (1,)), ((), ())), preferred_element_type=f32)


def fine_dot(dot, left, right):
    left_high, left_low = split(left)
    right_high, right_low = split(right)
    return dot(left_high, right_high) + (dot(left_high, right_low) + dot(left_low, right_high))


def newton_kernel(panel_ref, factor_ref, error_ref, tri_ref):
    count, order = panel_ref.shape[0], panel_ref.shape[1]
    rows = lax.broadcasted_iota(jnp.int32, (order, order), 0)
    cols = lax.broadcasted_iota(jnp.int32, (order, order), 1)
    eye = (rows == cols).astype(f32)
    half = jnp.where(rows > cols, 1.0, 0.5 * eye).astype(f32)

    for m in range(count):
        panel = panel_ref[m]
        scale = lax.rsqrt(jnp.sum(panel * panel, axis=1, keepdims=True))
        factor_ref[m] = panel * scale
        tri_ref[m] = eye * scale

    def coarse(carried):
        step, worst = carried
        worst = jnp.float32(0.0)
        for m in range(count):
            near = factor_ref[m].astype(bf16)
            lower = (dot_nt(near, near) - eye) * half
            size2 = jnp.sum(lower * lower)
            move = (lower * jnp.minimum(1.0, DAMP * lax.rsqrt(size2))).astype(bf16)
            factor_ref[m] -= dot_nn(move, near)
            tri_ref[m] -= dot_nn(move, tri_ref[m].astype(bf16))
            worst = jnp.maximum(worst, 2.0 * size2)
        return step + 1, worst

    lax.while_loop(
        lambda c: (c[0] < COARSE_STEPS) & (c[1] > COARSE * COARSE), coarse, (jnp.int32(0), jnp.float32(1e9))
    )
    for m in range(count):
        factor_ref[m] = fine_dot(dot_nn, tri_ref[m], panel_ref[m])

    def fine(carried):
        step, worst = carried
        worst = jnp.float32(0.0)
        for m in range(count):
            near = factor_ref[m]
            lower = (fine_dot(dot_nt, near, near) - eye) * half
            factor_ref[m] = near - fine_dot(dot_nn, lower, near)
            worst = jnp.maximum(worst, 2.0 * jnp.sum(lower * lower))
        return step + 1, worst

    _, worst = lax.while_loop(
        lambda c: (c[0] < FINE_STEPS) & (c[1] > FINE * FINE), fine, (jnp.int32(0), jnp.float32(1e9))
    )
    error_ref[...] = jnp.full(error_ref.shape, worst, f32)


def orthogonal_rows(panel):
    return pl.pallas_call(
        newton_kernel,
        out_shape=(jax.ShapeDtypeStruct(panel.shape, f32), jax.ShapeDtypeStruct((8, 128), f32)),
        in_specs=[pl.BlockSpec(memory_space=pltpu.VMEM)],
        out_specs=(pl.BlockSpec(memory_space=pltpu.VMEM), pl.BlockSpec(memory_space=pltpu.VMEM)),
        scratch_shapes=[pltpu.VMEM(panel.shape, f32)],
        cost_estimate=pl.CostEstimate(flops=10**9, bytes_accessed=10**6, transcendentals=0),
    )(panel)


def neighbours_ready(position, count):
    barrier = pltpu.get_barrier_semaphore()
    for away in (1, count - 1):
        peer = {"row": lax.rem(position + away, count)}
        pl.semaphore_signal(barrier, inc=1, device_id=peer, device_id_type=MESH)
    pl.semaphore_wait(barrier, 2)


def product_kernel(count, coupling_ref, product_ref, inbox, high_ref, low_ref, send_sem, recv_sem):
    position = lax.axis_index("row")
    batch, order = coupling_ref.shape[0], coupling_ref.shape[1]
    chunks = order // CHUNK
    neighbours_ready(position, count)

    @pl.when(position == 0)
    def _():
        rows = lax.broadcasted_iota(jnp.int32, (order, order), 0)
        cols = lax.broadcasted_iota(jnp.int32, (order, order), 1)
        for m in range(batch):
            inbox[m] = (rows == cols).astype(f32)

    for m in range(batch):
        high_ref[m], low_ref[m] = split(coupling_ref[m])

    def passing(step):
        m, rows = lax.div(step, chunks), pl.ds(pl.multiple_of(lax.rem(step, chunks) * CHUNK, CHUNK), CHUNK)
        copy = pltpu.make_async_remote_copy(
            src_ref=product_ref.at[m, rows],
            dst_ref=inbox.at[m, rows],
            send_sem=send_sem.at[step],
            recv_sem=recv_sem.at[step],
            device_id={"row": lax.rem(position + 1, count)},
            device_id_type=MESH,
        )
        return m, rows, copy

    def forward(step, unused):
        m, rows, copy = passing(step)

        @pl.when(position > 0)
        def _():
            copy.wait_recv()

        high, low = split(inbox[m, rows])
        product_ref[m, rows] = dot_nt(high, high_ref[m]) + (dot_nt(high, low_ref[m]) + dot_nt(low, high_ref[m]))

        @pl.when(position < count - 1)
        def _():
            copy.start()

        return unused

    def sent(step, unused):
        @pl.when(position < count - 1)
        def _():
            passing(step)[2].wait_send()

        return unused

    lax.fori_loop(0, batch * chunks, forward, 0)
    lax.fori_loop(0, batch * chunks, sent, 0)


def prefix_product(coupling):
    count, steps = lax.axis_size("row"), coupling.shape[0] * (coupling.shape[1] // CHUNK)
    return pl.pallas_call(
        lambda *refs: product_kernel(count, *refs),
        out_shape=jax.ShapeDtypeStruct(coupling.shape, f32),
        in_specs=[pl.BlockSpec(memory_space=pltpu.VMEM)],
        out_specs=pl.BlockSpec(memory_space=pltpu.VMEM),
        scratch_shapes=[
            pltpu.VMEM(coupling.shape, f32),
            pltpu.VMEM(coupling.shape, bf16),
            pltpu.VMEM(coupling.shape, bf16),
            pltpu.SemaphoreType.DMA((steps,)),
            pltpu.SemaphoreType.DMA((steps,)),
        ],
        compiler_params=pltpu.CompilerParams(collective_id=0, has_side_effects=True),
    )(coupling)


def finish_kernel(
    count, sections, factor_ref, coupling_ref, diag_ref, error_ref, new_ref, upper_ref, fault_ref,
    before, own_fault, row_fault, row_box, section_box, send_sem, recv_sem, flag_send, flag_recv,
):
    position, section = lax.axis_index("row"), lax.axis_index("section")
    batch, order = coupling_ref.shape[0], coupling_ref.shape[1]
    barrier = pltpu.get_barrier_semaphore()
    for k in range(1, count):
        peer = {"row": lax.rem(position + k, count)}
        pl.semaphore_signal(barrier, inc=1, device_id=peer, device_id_type=MESH)
    for k in range(1, sections):
        peer = {"section": lax.rem(section + k, sections)}
        pl.semaphore_signal(barrier, inc=1, device_id=peer, device_id_type=MESH)
    pl.semaphore_wait(barrier, count + sections - 2)

    copies = [
        pltpu.make_async_remote_copy(
            src_ref=factor_ref.at[m],
            dst_ref=before.at[m],
            send_sem=send_sem.at[m],
            recv_sem=recv_sem.at[m],
            device_id={"row": lax.rem(position + 1, count)},
            device_id_type=MESH,
        )
        for m in range(batch)
    ]

    @pl.when(position < count - 1)
    def _():
        for copy in copies:
            copy.start()

    rows = lax.broadcasted_iota(jnp.int32, (order, order), 0)
    cols = lax.broadcasted_iota(jnp.int32, (order, order), 1)

    @pl.when(position == 0)
    def _():
        for m in range(batch):
            before[m] = (rows == cols).astype(f32)

    for m in range(batch):
        upper_ref[m] = fine_dot(dot_nn, factor_ref[m], coupling_ref[m])
        new_ref[m] = fine_dot(dot_nt, fine_dot(dot_nn, factor_ref[m], diag_ref[m]), factor_ref[m])

    bad = jnp.where(error_ref[...] <= FINE * FINE, 0.0, 1.0)
    for m in range(batch):

        @pl.when(position > 0)
        def _():
            copies[m].wait_recv()

        full = fine_dot(dot_nt, upper_ref[m], before[m])
        upper_ref[m] = jnp.where(rows <= cols, full, 0.0)
        squares = full * full
        below2 = jnp.sum(jnp.where(rows > cols, squares, 0.0), axis=(0, 1), keepdims=True)
        all2 = jnp.sum(squares, axis=(0, 1), keepdims=True)
        least = jnp.min(jnp.where(rows == cols, full, jnp.inf), axis=(0, 1), keepdims=True)
        bad += jnp.where((below2 <= BELOW * BELOW * all2) & (least > 0.0), 0.0, 1.0)
    own_fault[...] = bad

    def exchange(source, box, axis, here, size, first):
        sends = [
            pltpu.make_async_remote_copy(
                src_ref=source,
                dst_ref=box.at[k - 1],
                send_sem=flag_send.at[first + k - 1],
                recv_sem=flag_recv.at[first + k - 1],
                device_id={axis: lax.rem(here + k, size)},
                device_id_type=MESH,
            )
            for k in range(1, size)
        ]
        for send in sends:
            send.start()
        for send in sends:
            send.wait()
        return source[...] + sum(box[k] for k in range(size - 1))

    row_fault[...] = exchange(own_fault, row_box, "row", position, count, 0)
    fault_ref[...] = exchange(row_fault, section_box, "section", section, sections, count - 1)

    @pl.when(position < count - 1)
    def _():
        for copy in copies:
            copy.wait_send()


def finish(factor, coupling, diagonal, error):
    count, sections = lax.axis_size("row"), lax.axis_size("section")
    batch = coupling.shape[0]
    flags = count + sections - 2
    vmem = pl.BlockSpec(memory_space=pltpu.VMEM)
    return pl.pallas_call(
        lambda *refs: finish_kernel(count, sections, *refs),
        out_shape=(
            jax.ShapeDtypeStruct(coupling.shape, f32),
            jax.ShapeDtypeStruct(coupling.shape, f32),
            jax.ShapeDtypeStruct(error.shape, f32),
        ),
        in_specs=[vmem] * 4,
        out_specs=(vmem, vmem, vmem),
        scratch_shapes=[
            pltpu.VMEM(coupling.shape, f32),
            pltpu.VMEM(error.shape, f32),
            pltpu.VMEM(error.shape, f32),
            pltpu.VMEM((count - 1, *error.shape), f32),
            pltpu.VMEM((sections - 1, *error.shape), f32),
            pltpu.SemaphoreType.DMA((batch,)),
            pltpu.SemaphoreType.DMA((batch,)),
            pltpu.SemaphoreType.DMA((flags,)),
            pltpu.SemaphoreType.DMA((flags,)),
        ],
        compiler_params=pltpu.CompilerParams(collective_id=1, has_side_effects=True),
    )(factor, coupling, diagonal, error)


def shards(diag_blocks, coupling_blocks):
    if diag_blocks.shape[2] != 1:
        return chain(diag_blocks, coupling_blocks)
    diagonal, coupling = diag_blocks[0, :, 0], coupling_blocks[0, :, 0]
    factor, error = orthogonal_rows(prefix_product(coupling))
    new_diag, upper, faults = finish(factor, coupling, diagonal, error)
    return lax.cond(
        faults[0, 0] == 0.0,
        lambda: (new_diag[None, :, None], upper[None, :, None]),
        lambda: chain(diag_blocks, coupling_blocks),
    )


def shifted(block, axis, distance):
    devices = range(lax.axis_size(axis))
    route = [(i - distance, i) for i in devices if i - distance in devices]
    return lax.ppermute(block, axis, route)


def product(left, right):
    return jnp.dot(left, right, precision=highest, preferred_element_type=jnp.float32)


def qfactor(panel_now):
    def one_pass(_, carried):
        panel, upper = carried
        lower = jnp.linalg.cholesky(product(panel.T, panel))
        return jax.scipy.linalg.solve_triangular(lower, panel.T, lower=True).T, product(lower.T, upper)

    return lax.fori_loop(0, 2, one_pass, (panel_now, jnp.eye(panel_now.shape[0], dtype=f32)))


def segment(panel_now, diagonal):
    orthogonal, upper_part = qfactor(panel_now)
    new_diag = [product(product(orthogonal.T, diagonal[0]), orthogonal)]
    triangles = [upper_part]
    return (jnp.stack(new_diag), jnp.stack(triangles), orthogonal)


def pass_on(outgoing):
    return shifted(outgoing, "row", 1)


def chain(diag_blocks, coupling_blocks):
    diagonal = diag_blocks[0]
    coupling = coupling_blocks[0]
    batch_count = diagonal.shape[0]
    row_count = lax.axis_size("row")
    position = lax.axis_index("row")
    leading = position == 0

    def opening(incoming, own_first):
        made = product(own_first, incoming)
        return jnp.where(leading, own_first, made)

    new_start = jnp.zeros_like(diagonal)
    tri_start = jnp.zeros_like(diagonal)

    def process_one(incoming, new_all, tri_all, clipped):
        diag_now = lax.dynamic_index_in_dim(diagonal, clipped, 0, keepdims=False)
        coupling_now = lax.dynamic_index_in_dim(coupling, clipped, 0, keepdims=False)
        first_panel = opening(incoming, coupling_now[0])
        new_diag, triangles, last_factor = segment(first_panel, diag_now)
        new_all = lax.dynamic_update_index_in_dim(new_all, new_diag, clipped, 0)
        tri_all = lax.dynamic_update_index_in_dim(tri_all, triangles, clipped, 0)
        return (new_all, tri_all, last_factor)

    def round_step(step_number, carried):
        incoming, new_all, tri_all, outgoing = carried
        batch_index = step_number - position
        active = (batch_index >= 0) & (batch_index < batch_count)
        clipped = jnp.clip(batch_index, 0, batch_count - 1)
        new_all, tri_all, outgoing = lax.cond(
            active,
            lambda: process_one(incoming, new_all, tri_all, clipped),
            lambda: (new_all, tri_all, outgoing),
        )
        return (pass_on(outgoing), new_all, tri_all, outgoing)

    message_start = jnp.zeros_like(coupling[0, 0])
    carried = lax.fori_loop(
        0,
        row_count + batch_count - 1,
        round_step,
        (message_start, new_start, tri_start, message_start),
    )
    return (carried[1][None], carried[2][None])


def solution(mesh):
    placed = (P("section", None, "row", None, None), P("section", None, "row", None, None))
    return jax.shard_map(
        shards,
        mesh=mesh,
        in_specs=placed,
        out_specs=(P("section", None, "row", None, None), P("section", None, "row", None, None)),
        check_vma=False,
    )
```

```python
import jax
import jax.numpy as jnp
from jax import lax
from jax.experimental import pallas as pl
from jax.experimental.pallas import tpu as pltpu
from jax.sharding import PartitionSpec as P

highest = lax.Precision.HIGHEST
f32, bf16 = jnp.float32, jnp.bfloat16
MESH = pl.DeviceIdType.MESH
CHUNK = 32

DAMP, COARSE, FINE = 5.0, 0.5, 2e-3
COARSE_STEPS, FINE_STEPS = 48, 8
BELOW = 5e-5


def split(value):
    high = value.astype(bf16)
    return high, (value - high.astype(f32)).astype(bf16)


def dot_nn(left, right):
    return lax.dot_general(left, right, (((1,), (0,)), ((), ())), preferred_element_type=f32)


def dot_nt(left, right):
    return lax.dot_general(left, right, (((1,), (1,)), ((), ())), preferred_element_type=f32)


def fine_dot(dot, left, right):
    left_high, left_low = split(left)
    right_high, right_low = split(right)
    return dot(left_high, right_high) + (dot(left_high, right_low) + dot(left_low, right_high))


def newton_kernel(panel_ref, factor_ref, error_ref, tri_ref):
    count, order = panel_ref.shape[0], panel_ref.shape[1]
    rows = lax.broadcasted_iota(jnp.int32, (order, order), 0)
    cols = lax.broadcasted_iota(jnp.int32, (order, order), 1)
    eye = (rows == cols).astype(f32)
    half = jnp.where(rows > cols, 1.0, 0.5 * eye).astype(f32)

    for m in range(count):
        panel = panel_ref[m]
        scale = lax.rsqrt(jnp.sum(panel * panel, axis=1, keepdims=True))
        factor_ref[m] = panel * scale
        tri_ref[m] = eye * scale

    def coarse(carried):
        step, worst = carried
        worst = jnp.float32(0.0)
        for m in range(count):
            near = factor_ref[m].astype(bf16)
            lower = (dot_nt(near, near) - eye) * half
            size2 = jnp.sum(lower * lower)
            move = (lower * jnp.minimum(1.0, DAMP * lax.rsqrt(size2))).astype(bf16)
            factor_ref[m] -= dot_nn(move, near)
            tri_ref[m] -= dot_nn(move, tri_ref[m].astype(bf16))
            worst = jnp.maximum(worst, 2.0 * size2)
        return step + 1, worst

    lax.while_loop(
        lambda c: (c[0] < COARSE_STEPS) & (c[1] > COARSE * COARSE), coarse, (jnp.int32(0), jnp.float32(1e9))
    )
    for m in range(count):
        factor_ref[m] = fine_dot(dot_nn, tri_ref[m], panel_ref[m])

    def fine(carried):
        step, worst = carried
        worst = jnp.float32(0.0)
        for m in range(count):
            near = factor_ref[m]
            lower = (fine_dot(dot_nt, near, near) - eye) * half
            factor_ref[m] = near - fine_dot(dot_nn, lower, near)
            worst = jnp.maximum(worst, 2.0 * jnp.sum(lower * lower))
        return step + 1, worst

    _, worst = lax.while_loop(
        lambda c: (c[0] < FINE_STEPS) & (c[1] > FINE * FINE), fine, (jnp.int32(0), jnp.float32(1e9))
    )
    error_ref[...] = jnp.full(error_ref.shape, worst, f32)


def orthogonal_rows(panel):
    return pl.pallas_call(
        newton_kernel,
        out_shape=(jax.ShapeDtypeStruct(panel.shape, f32), jax.ShapeDtypeStruct((8, 128), f32)),
        in_specs=[pl.BlockSpec(memory_space=pltpu.VMEM)],
        out_specs=(pl.BlockSpec(memory_space=pltpu.VMEM), pl.BlockSpec(memory_space=pltpu.VMEM)),
        scratch_shapes=[pltpu.VMEM(panel.shape, f32)],
        cost_estimate=pl.CostEstimate(flops=10**9, bytes_accessed=10**6, transcendentals=0),
    )(panel)


def neighbours_ready(position, count):
    barrier = pltpu.get_barrier_semaphore()
    for away in (1, count - 1):
        peer = {"row": lax.rem(position + away, count)}
        pl.semaphore_signal(barrier, inc=1, device_id=peer, device_id_type=MESH)
    pl.semaphore_wait(barrier, 2)


def product_kernel(count, coupling_ref, product_ref, inbox, high_ref, low_ref, send_sem, recv_sem):
    position = lax.axis_index("row")
    batch, order = coupling_ref.shape[0], coupling_ref.shape[1]
    chunks = order // CHUNK
    neighbours_ready(position, count)

    def passing(step):
        m, rows = lax.div(step, chunks), pl.ds(pl.multiple_of(lax.rem(step, chunks) * CHUNK, CHUNK), CHUNK)
        copy = pltpu.make_async_remote_copy(
            src_ref=product_ref.at[m, rows],
            dst_ref=inbox.at[m, rows],
            send_sem=send_sem.at[step],
            recv_sem=recv_sem.at[step],
            device_id={"row": lax.rem(position + 1, count)},
            device_id_type=MESH,
        )
        return m, rows, copy

    def forward(step, unused):
        m, rows, copy = passing(step)
        copy.wait_recv()
        high, low = split(inbox[m, rows])
        both = dot_nn(jnp.concatenate([high, low], axis=0), high_ref[m])
        product_ref[m, rows] = both[:CHUNK] + (both[CHUNK:] + dot_nn(high, low_ref[m]))

        @pl.when(position < count - 1)
        def _():
            copy.start()

        return unused

    def first(step, unused):
        passing(step)[2].start()
        return unused

    def sent(step, unused):
        @pl.when(position < count - 1)
        def _():
            passing(step)[2].wait_send()

        return unused

    @pl.when(position == 0)
    def _():
        for m in range(batch):
            product_ref[m] = coupling_ref[m].T
        lax.fori_loop(0, batch * chunks, first, 0)

    @pl.when(position > 0)
    def _():
        for m in range(batch):
            high_ref[m], low_ref[m] = split(coupling_ref[m].T)
        lax.fori_loop(0, batch * chunks, forward, 0)

    lax.fori_loop(0, batch * chunks, sent, 0)


def prefix_product(coupling):
    count, steps = lax.axis_size("row"), coupling.shape[0] * (coupling.shape[1] // CHUNK)
    return pl.pallas_call(
        lambda *refs: product_kernel(count, *refs),
        out_shape=jax.ShapeDtypeStruct(coupling.shape, f32),
        in_specs=[pl.BlockSpec(memory_space=pltpu.VMEM)],
        out_specs=pl.BlockSpec(memory_space=pltpu.VMEM),
        scratch_shapes=[
            pltpu.VMEM(coupling.shape, f32),
            pltpu.VMEM(coupling.shape, bf16),
            pltpu.VMEM(coupling.shape, bf16),
            pltpu.SemaphoreType.DMA((steps,)),
            pltpu.SemaphoreType.DMA((steps,)),
        ],
        compiler_params=pltpu.CompilerParams(collective_id=0, has_side_effects=True),
    )(coupling)


def finish_kernel(
    count, sections, factor_ref, coupling_ref, diag_ref, error_ref, new_ref, upper_ref, fault_ref,
    before, own_fault, row_fault, row_box, section_box, send_sem, recv_sem, flag_send, flag_recv,
):
    position, section = lax.axis_index("row"), lax.axis_index("section")
    batch, order = coupling_ref.shape[0], coupling_ref.shape[1]
    barrier = pltpu.get_barrier_semaphore()
    for k in range(1, count):
        peer = {"row": lax.rem(position + k, count)}
        pl.semaphore_signal(barrier, inc=1, device_id=peer, device_id_type=MESH)
    for k in range(1, sections):
        peer = {"section": lax.rem(section + k, sections)}
        pl.semaphore_signal(barrier, inc=1, device_id=peer, device_id_type=MESH)
    pl.semaphore_wait(barrier, count + sections - 2)

    copies = [
        pltpu.make_async_remote_copy(
            src_ref=factor_ref.at[m],
            dst_ref=before.at[m],
            send_sem=send_sem.at[m],
            recv_sem=recv_sem.at[m],
            device_id={"row": lax.rem(position + 1, count)},
            device_id_type=MESH,
        )
        for m in range(batch)
    ]

    @pl.when(position < count - 1)
    def _():
        for copy in copies:
            copy.start()

    rows = lax.broadcasted_iota(jnp.int32, (order, order), 0)
    cols = lax.broadcasted_iota(jnp.int32, (order, order), 1)

    @pl.when(position == 0)
    def _():
        for m in range(batch):
            before[m] = (rows == cols).astype(f32)

    for m in range(batch):
        upper_ref[m] = fine_dot(dot_nn, factor_ref[m], coupling_ref[m])
        new_ref[m] = fine_dot(dot_nt, fine_dot(dot_nn, factor_ref[m], diag_ref[m]), factor_ref[m])

    bad = jnp.where(error_ref[...] <= FINE * FINE, 0.0, 1.0)
    for m in range(batch):

        @pl.when(position > 0)
        def _():
            copies[m].wait_recv()

        full = fine_dot(dot_nt, upper_ref[m], before[m])
        upper_ref[m] = jnp.where(rows <= cols, full, 0.0)
        squares = full * full
        below2 = jnp.sum(jnp.where(rows > cols, squares, 0.0), axis=(0, 1), keepdims=True)
        all2 = jnp.sum(squares, axis=(0, 1), keepdims=True)
        least = jnp.min(jnp.where(rows == cols, full, jnp.inf), axis=(0, 1), keepdims=True)
        bad += jnp.where((below2 <= BELOW * BELOW * all2) & (least > 0.0), 0.0, 1.0)
    own_fault[...] = bad

    def exchange(source, box, axis, here, size, first):
        sends = [
            pltpu.make_async_remote_copy(
                src_ref=source,
                dst_ref=box.at[k - 1],
                send_sem=flag_send.at[first + k - 1],
                recv_sem=flag_recv.at[first + k - 1],
                device_id={axis: lax.rem(here + k, size)},
                device_id_type=MESH,
            )
            for k in range(1, size)
        ]
        for send in sends:
            send.start()
        for send in sends:
            send.wait()
        return source[...] + sum(box[k] for k in range(size - 1))

    row_fault[...] = exchange(own_fault, row_box, "row", position, count, 0)
    fault_ref[...] = exchange(row_fault, section_box, "section", section, sections, count - 1)

    @pl.when(position < count - 1)
    def _():
        for copy in copies:
            copy.wait_send()


def finish(factor, coupling, diagonal, error):
    count, sections = lax.axis_size("row"), lax.axis_size("section")
    batch = coupling.shape[0]
    flags = count + sections - 2
    vmem = pl.BlockSpec(memory_space=pltpu.VMEM)
    return pl.pallas_call(
        lambda *refs: finish_kernel(count, sections, *refs),
        out_shape=(
            jax.ShapeDtypeStruct(coupling.shape, f32),
            jax.ShapeDtypeStruct(coupling.shape, f32),
            jax.ShapeDtypeStruct(error.shape, f32),
        ),
        in_specs=[vmem] * 4,
        out_specs=(vmem, vmem, vmem),
        scratch_shapes=[
            pltpu.VMEM(coupling.shape, f32),
            pltpu.VMEM(error.shape, f32),
            pltpu.VMEM(error.shape, f32),
            pltpu.VMEM((count - 1, *error.shape), f32),
            pltpu.VMEM((sections - 1, *error.shape), f32),
            pltpu.SemaphoreType.DMA((batch,)),
            pltpu.SemaphoreType.DMA((batch,)),
            pltpu.SemaphoreType.DMA((flags,)),
            pltpu.SemaphoreType.DMA((flags,)),
        ],
        compiler_params=pltpu.CompilerParams(collective_id=1, has_side_effects=True),
    )(factor, coupling, diagonal, error)


def shards(diag_blocks, coupling_blocks):
    if diag_blocks.shape[2] != 1:
        return chain(diag_blocks, coupling_blocks)
    diagonal, coupling = diag_blocks[0, :, 0], coupling_blocks[0, :, 0]
    factor, error = orthogonal_rows(prefix_product(coupling))
    new_diag, upper, faults = finish(factor, coupling, diagonal, error)
    return lax.cond(
        faults[0, 0] == 0.0,
        lambda: (new_diag[None, :, None], upper[None, :, None]),
        lambda: chain(diag_blocks, coupling_blocks),
    )


def shifted(block, axis, distance):
    devices = range(lax.axis_size(axis))
    route = [(i - distance, i) for i in devices if i - distance in devices]
    return lax.ppermute(block, axis, route)


def product(left, right):
    return jnp.dot(left, right, precision=highest, preferred_element_type=jnp.float32)


def qfactor(panel_now):
    def one_pass(_, carried):
        panel, upper = carried
        lower = jnp.linalg.cholesky(product(panel.T, panel))
        return jax.scipy.linalg.solve_triangular(lower, panel.T, lower=True).T, product(lower.T, upper)

    return lax.fori_loop(0, 2, one_pass, (panel_now, jnp.eye(panel_now.shape[0], dtype=f32)))


def segment(panel_now, diagonal):
    orthogonal, upper_part = qfactor(panel_now)
    new_diag = [product(product(orthogonal.T, diagonal[0]), orthogonal)]
    triangles = [upper_part]
    return (jnp.stack(new_diag), jnp.stack(triangles), orthogonal)


def pass_on(outgoing):
    return shifted(outgoing, "row", 1)


def chain(diag_blocks, coupling_blocks):
    diagonal = diag_blocks[0]
    coupling = coupling_blocks[0]
    batch_count = diagonal.shape[0]
    row_count = lax.axis_size("row")
    position = lax.axis_index("row")
    leading = position == 0

    def opening(incoming, own_first):
        made = product(own_first, incoming)
        return jnp.where(leading, own_first, made)

    new_start = jnp.zeros_like(diagonal)
    tri_start = jnp.zeros_like(diagonal)

    def process_one(incoming, new_all, tri_all, clipped):
        diag_now = lax.dynamic_index_in_dim(diagonal, clipped, 0, keepdims=False)
        coupling_now = lax.dynamic_index_in_dim(coupling, clipped, 0, keepdims=False)
        first_panel = opening(incoming, coupling_now[0])
        new_diag, triangles, last_factor = segment(first_panel, diag_now)
        new_all = lax.dynamic_update_index_in_dim(new_all, new_diag, clipped, 0)
        tri_all = lax.dynamic_update_index_in_dim(tri_all, triangles, clipped, 0)
        return (new_all, tri_all, last_factor)

    def round_step(step_number, carried):
        incoming, new_all, tri_all, outgoing = carried
        batch_index = step_number - position
        active = (batch_index >= 0) & (batch_index < batch_count)
        clipped = jnp.clip(batch_index, 0, batch_count - 1)
        new_all, tri_all, outgoing = lax.cond(
            active,
            lambda: process_one(incoming, new_all, tri_all, clipped),
            lambda: (new_all, tri_all, outgoing),
        )
        return (pass_on(outgoing), new_all, tri_all, outgoing)

    message_start = jnp.zeros_like(coupling[0, 0])
    carried = lax.fori_loop(
        0,
        row_count + batch_count - 1,
        round_step,
        (message_start, new_start, tri_start, message_start),
    )
    return (carried[1][None], carried[2][None])


def solution(mesh):
    placed = (P("section", None, "row", None, None), P("section", None, "row", None, None))
    return jax.shard_map(
        shards,
        mesh=mesh,
        in_specs=placed,
        out_specs=(P("section", None, "row", None, None), P("section", None, "row", None, None)),
        check_vma=False,
    )
```
